32 devices in a mesh: mem: 4 (over z), reg: 8 (over y, x, core).
Axes of the slice: x: 2, y: 2, z: 4, core: 2. Of those that a mesh axis runs over, the one named last changes fastest.
Arguments:
- member_values: float32 [40, 32768], P('mem', 'reg'), may hold values from -6 to 6
- obs_value: float32 [32768], P('reg'), may hold values from -6 to 6
- obs_weight: float32 [32768], P('reg'), may hold values from 0.25 to 4
- obs_cell: int32 [32768], P('reg'), may hold values from -1 to 15359, as said below
Outputs:
- deviation: float32 [40, 15360], P('mem', 'reg')
- departure: float32 [15360], P('reg')
- variance: float32 [15360], P('reg')
- error_variance: float32 [15360], P('reg')
- obs_total: int32 [15360], P('reg')
The draws below stay inside these ranges and needn't reach their ends.
Inputs may be any that keep to these rules, and one draw needn't show every extreme that they name: `obs_cell`: cell c is owned by region c // 1920. The 4096 slots of one region are 8 blocks of 512 slots, block r holding only cells owned by region r, live slots first and -1 in the empty ones. Every block has at least 128 live slots; one owner's block is full in every region.
All inputs are finite; a program needn't handle non-finite values.
Results may differ from the reference program's by a relative error of at most 0.0003.
Values sent between devices are 32-bit elements; how exact they have to be, the bound alone decides.
No kernel may reach another device: no remote copies, remote signals or barrier semaphores. Data moves between devices by JAX's collectives and lax.ppermute only.
A program may use at most 64 MiB of HBM per device.

```python
import math
import jax
import jax.numpy as jnp

CAP = 512
CELL_DEV = 1920
MEMBERS = 40
OBS = 32768
CELLS = 15360
N_REG = 8


def draw_obs_cell(key, part):
    subkeys = jax.random.split(jax.random.fold_in(key, 7), 4)
    dense_owner = jax.random.randint(subkeys[0], (), 0, N_REG)
    block_counts = jax.random.randint(subkeys[1], (N_REG, N_REG), CAP // 4, CAP + 1)
    owner_ids = jnp.arange(N_REG, dtype=jnp.int32)
    block_counts = jnp.where(owner_ids[None, :] == dense_owner, CAP, block_counts)
    slot_ids = jnp.arange(CAP, dtype=jnp.int32)
    live = slot_ids[None, None, :] < block_counts[:, :, None]
    factor_one = jax.random.randint(subkeys[2], (N_REG, N_REG, CAP), 0, CELL_DEV)
    factor_two = jax.random.randint(subkeys[3], (N_REG, N_REG, CAP), 0, CELL_DEV)
    local_cell = factor_one * factor_two // CELL_DEV
    local_cell = (local_cell * 7919 + 101) % CELL_DEV
    cell_ids = owner_ids[None, :, None] * CELL_DEV + local_cell
    cell_ids = jnp.where(live, cell_ids, -1)
    return cell_ids.reshape(-1).astype(jnp.int32)


def levels(rng, extent, pieces, least, largest):
    def one(position, shards_of):
        draws = jax.random.uniform(jax.random.fold_in(jax.random.fold_in(rng, 6), position), (shards_of,), jnp.float32, least / len(pieces), largest / len(pieces))
        return jnp.repeat(jnp.exp(draws), extent[position] // shards_of).reshape((-1,) + (1,) * (len(extent) - position - 1))

    loudness = one(*pieces[0])
    for cut in pieces[1:]:
        loudness = loudness * one(*cut)
    return loudness


def bell_draw(key, extent, spread, most, shards=(), kind=jnp.bfloat16):
    loudness = levels(key, extent, shards, -0.22, 0.18) if shards else 1.0
    result = jax.random.normal(key, extent, jnp.float32) * spread * loudness
    return jnp.minimum(jnp.maximum(result, -most), most).astype(kind)


def setup_inputs(seed: int = 0) -> dict:
    streams_of = jax.random.split(jax.random.key(seed), 5)
    return {
        "member_values": bell_draw(streams_of[0], (MEMBERS, OBS), 1.0, 6.0, ((0, 4), (1, 8)), jnp.float32),
        "obs_value": bell_draw(streams_of[1], (OBS,), 1.0, 6.0, ((0, 8),), jnp.float32),
        "obs_weight": jnp.clip(jnp.exp(math.log(4.0) - 2.7725887 * jax.random.uniform(streams_of[2], (OBS,), jnp.float32) ** levels(streams_of[2], (OBS,), ((0, 8),), -0.2, 0.2)), 0.25, 4.0),
        "obs_cell": draw_obs_cell(jax.random.fold_in(streams_of[4], 71), 0),
    }


def reference(member_values, obs_value, obs_weight, obs_cell):
    live = obs_cell >= 0
    weight = jnp.where(live, obs_weight, jnp.float32(0.0))
    cell_ids = jnp.where(live, obs_cell, 0).astype(jnp.int32)
    filled_flag = live.astype(jnp.float32)
    columns = jnp.concatenate([member_values * weight[None, :], (weight * obs_value)[None, :], weight[None, :], filled_flag[None, :]], 0)
    cell_sums = jax.vmap(lambda single: jax.ops.segment_sum(single, cell_ids, num_segments=CELLS))(columns)
    counted = cell_sums[MEMBERS + 2]
    filled = counted > 0
    weight_total = jnp.where(filled, cell_sums[MEMBERS + 1], jnp.float32(1.0))
    superob = cell_sums[:MEMBERS] / weight_total[None, :]
    observed_mean = cell_sums[MEMBERS] / weight_total
    ens_mean = jnp.sum(superob, 0) / MEMBERS
    deviation = superob - ens_mean[None, :]
    variance = jnp.sum(deviation * deviation, 0) / (MEMBERS - 1)
    departure = observed_mean - ens_mean
    error_variance = jnp.where(filled, 1.0 / weight_total, jnp.float32(0.0))
    return deviation, departure, variance, error_variance, counted.astype(jnp.int32)
```

```python
import functools
import jax
import jax.numpy as jnp
from jax import lax
from jax.experimental import pallas as pl
from jax.experimental.pallas import tpu as pltpu
from jax.sharding import PartitionSpec as P

CELL_DEV = 1920
LANES = 128
WIDE = 256


def round_up(size, unit):
    return -(-size // unit) * unit


def block_rows(members):
    rows = round_up(members + 2, 4)
    return rows, rows // 8 * 8


def pack_kernel(members, regions, chunks, value_ref, obs_ref, weight_ref, cell_ref, same_ref, other_ref):
    me = lax.axis_index("reg")
    rows, whole = block_rows(members)
    rest = rows - whole
    for step in range(regions):
        owner = me ^ step
        out_ref = other_ref if step % 2 else same_ref
        for j in range(chunks):
            line = owner * chunks + j
            values = value_ref[:, pl.ds(pl.multiple_of(line * LANES, LANES), LANES)]
            cell = cell_ref[pl.ds(line, 1), :]
            live = cell >= 0
            weight = jnp.where(live, weight_ref[pl.ds(line, 1), :], 0.0)
            local = jnp.where(live, cell - owner * CELL_DEV, -1).astype(jnp.float32)
            innovation = (values - obs_ref[pl.ds(line, 1), :]) * weight
            tail = whole * chunks + j * rest
            out_ref[step // 2, pl.ds(j * whole, whole), :] = innovation[:whole]
            out_ref[step // 2, pl.ds(tail, members - whole), :] = innovation[whole:]
            out_ref[step // 2, pl.ds(tail + members - whole, 1), :] = weight
            out_ref[step // 2, pl.ds(tail + members - whole + 1, 1), :] = local


def bin_kernel(members, chunks, groups, in_refs, dev_ref, moment_ref, error_ref, count_ref, acc_ref):
    rows, whole = block_rows(members)
    rest = rows - whole
    pad = round_up(rows, 16)
    low_iota = lax.broadcasted_iota(jnp.int32, (WIDE, LANES), 0)
    row_iota = lax.broadcasted_iota(jnp.int32, (pad, LANES), 0)
    blocks = [(ref, b) for ref, picks in in_refs for b in picks]
    for n, (ref, b) in enumerate(blocks):
        parts, lows, highs = [], [], []
        for j in range(chunks):
            tail = whole * chunks + j * rest
            values = jnp.concatenate(
                [
                    ref[b, pl.ds(j * whole, whole), :],
                    ref[b, pl.ds(tail, rest), :],
                    jnp.zeros((pad - rows, LANES), jnp.float32),
                ],
                0,
            )
            cell = ref[b, pl.ds(tail + members - whole + 1, 1), :].astype(jnp.int32)
            live = (cell >= 0).astype(jnp.float32)
            values = jnp.where(row_iota == members + 1, live, values)
            top = values.astype(jnp.bfloat16)
            left_over = values - top.astype(jnp.float32)
            middle = left_over.astype(jnp.bfloat16)
            bottom = (left_over - middle.astype(jnp.float32)).astype(jnp.bfloat16)
            parts.append(jnp.concatenate([top, middle, bottom], 0))
            high = lax.shift_right_arithmetic(cell, 8)
            highs.append(jnp.broadcast_to(high, (3 * pad, LANES)))
            lows.append((low_iota == (cell & (WIDE - 1))).astype(jnp.float32).astype(jnp.bfloat16))
        part = jnp.concatenate(parts, 1)
        high = jnp.concatenate(highs, 1)
        low = jnp.concatenate(lows, 1)
        left = jnp.concatenate(
            [jnp.where(high == g, part, jnp.zeros_like(part)) for g in range(groups)], 0
        )
        product = lax.dot_general(
            left, low, (((1,), (1,)), ((), ())), preferred_element_type=jnp.float32
        )
        if n == 0:
            acc_ref[...] = product
        else:
            acc_ref[...] += product
    for g in range(groups):
        start, width = g * WIDE, min(WIDE, CELL_DEV - g * WIDE)
        base = g * 3 * pad
        sums = (
            acc_ref[pl.ds(base, pad), :width]
            + acc_ref[pl.ds(base + pad, pad), :width]
            + acc_ref[pl.ds(base + 2 * pad, pad), :width]
        )
        counted = sums[members + 1 : members + 2]
        filled = counted > 0
        total = jnp.where(filled, sums[members : members + 1], 1.0)
        deviation = sums[:members] / total
        moment = jnp.sum(deviation, 0, keepdims=True)
        centred = deviation - moment / members
        spread = jnp.sum(centred * centred, 0, keepdims=True)
        error = jnp.where(filled, 1.0 / total, 0.0)
        count = counted.astype(jnp.int32)
        dev_ref[:, start : start + width] = deviation
        for j in range(width // LANES):
            line, cut = start // LANES + j, slice(j * LANES, (j + 1) * LANES)
            moment_ref[0, line : line + 1, :] = moment[:, cut]
            moment_ref[1, line : line + 1, :] = spread[:, cut]
            error_ref[line : line + 1, :] = error[:, cut]
            count_ref[line : line + 1, :] = count[:, cut]


def near(array):
    return pltpu.with_memory_space_constraint(array, pltpu.VMEM)


def bin_call(members, chunks, arrays):
    groups = -(-CELL_DEV // WIDE)
    pad = round_up(block_rows(members)[0], 16)

    def body(*refs):
        pairs = list(zip(refs, [picks for _, picks in arrays]))
        bin_kernel(members, chunks, groups, pairs, *refs[len(arrays) :])

    lines = CELL_DEV // LANES
    return pl.pallas_call(
        body,
        out_shape=[
            pltpu.VMEM((members, CELL_DEV), jnp.float32),
            pltpu.VMEM((2, lines, LANES), jnp.float32),
            pltpu.VMEM((lines, LANES), jnp.float32),
            pltpu.VMEM((lines, LANES), jnp.int32),
        ],
        scratch_shapes=[pltpu.VMEM((groups * 3 * pad, WIDE), jnp.float32)],
    )(*[near(array) for array, _ in arrays])


def final_kernel(
    total, dev_ref, mine_ref, theirs_ref, error_in, count_in, out_ref, departure_ref, variance_ref, error_ref, count_ref
):
    half = total // 2
    moment = mine_ref[0] + theirs_ref[0]
    gap = mine_ref[0] - theirs_ref[0]
    spread = mine_ref[1] + theirs_ref[1] + gap * gap / (2 * half)
    mean = moment / total
    departure_ref[...] = -mean
    variance_ref[...] = spread / (total - 1)
    error_ref[...] = error_in[...]
    count_ref[...] = count_in[...]
    for j in range(CELL_DEV // LANES):
        cut = slice(j * LANES, (j + 1) * LANES)
        out_ref[:, cut] = dev_ref[:, cut] - mean[j : j + 1]


def merge(mine, theirs, each):
    gap = mine[0] - theirs[0]
    return jnp.stack([mine[0] + theirs[0], mine[1] + theirs[1] + gap * gap / (2 * each)])


def shards(member_values, obs_value, obs_weight, obs_cell):
    regions = lax.axis_size("reg")
    groups = lax.axis_size("mem")
    members, slots = member_values.shape
    chunks = slots // regions // LANES
    chips = regions // 2
    f32 = functools.partial(jax.ShapeDtypeStruct, dtype=jnp.float32)
    lines = (slots // LANES, LANES)
    same, other = pl.pallas_call(
        functools.partial(pack_kernel, members, regions, chunks),
        out_shape=[pltpu.VMEM((chips, chunks * block_rows(members)[0], LANES), jnp.float32)] * 2,
    )(member_values, obs_value.reshape(lines), obs_weight.reshape(lines), obs_cell.reshape(lines))
    partner = lax.ppermute(other, "reg", [(i, i ^ 1) for i in range(regions)])
    arrays = [(same, (0,)), (partner, (0,))]
    for k in range(chips - 1, 0, -1):
        sent = jnp.stack([same[k], partner[k]])
        arrays.append((lax.ppermute(sent, "reg", [(i, i ^ (2 * k)) for i in range(regions)]), (0, 1)))
    deviation, moments, error_variance, obs_total = bin_call(members, chunks, arrays)
    each, reach = members, 1
    while 2 * reach < groups:
        theirs = lax.ppermute(moments, "mem", [(i, i ^ reach) for i in range(groups)])
        moments = merge(moments, theirs, each)
        each, reach = 2 * each, 2 * reach
    theirs = lax.ppermute(moments, "mem", [(i, i ^ reach) for i in range(groups)])
    cells = (CELL_DEV // LANES, LANES)
    outs = pl.pallas_call(
        functools.partial(final_kernel, members * groups),
        out_shape=[f32((members, CELL_DEV)), f32(cells), f32(cells), f32(cells), jax.ShapeDtypeStruct(cells, jnp.int32)],
    )(*[near(a) for a in (deviation, moments, theirs, error_variance, obs_total)])
    return (outs[0], *[out.reshape(-1) for out in outs[1:]])


def solution(mesh):
    return jax.shard_map(
        shards,
        mesh=mesh,
        in_specs=(P("mem", "reg"), P("reg"), P("reg"), P("reg")),
        out_specs=(P("mem", "reg"), P("reg"), P("reg"), P("reg"), P("reg")),
        check_vma=False,
    )
```

```python
import functools
import jax
import jax.numpy as jnp
from jax import lax
from jax.experimental import pallas as pl
from jax.experimental.pallas import tpu as pltpu
from jax.sharding import PartitionSpec as P

CELL_DEV = 1920
LANES = 128
WIDE = 256


def round_up(size, unit):
    return -(-size // unit) * unit


def block_rows(members):
    rows = round_up(members + 2, 4)
    return rows, rows // 8 * 8


def pack_kernel(members, regions, chunks, value_ref, obs_ref, weight_ref, cell_ref, same_ref, other_ref):
    me = lax.axis_index("reg")
    rows, whole = block_rows(members)
    rest = rows - whole
    for step in range(regions):
        owner = me ^ step
        out_ref = other_ref if (step % 2) ^ (step > 1) else same_ref
        for j in range(chunks):
            line = owner * chunks + j
            values = value_ref[:, pl.ds(pl.multiple_of(line * LANES, LANES), LANES)]
            cell = cell_ref[pl.ds(line, 1), :]
            live = cell >= 0
            weight = jnp.where(live, weight_ref[pl.ds(line, 1), :], 0.0)
            local = jnp.where(live, cell - owner * CELL_DEV, -1).astype(jnp.float32)
            innovation = (values - obs_ref[pl.ds(line, 1), :]) * weight
            tail = whole * chunks + j * rest
            out_ref[step // 2, pl.ds(j * whole, whole), :] = innovation[:whole]
            out_ref[step // 2, pl.ds(tail, members - whole), :] = innovation[whole:]
            out_ref[step // 2, pl.ds(tail + members - whole, 1), :] = weight
            out_ref[step // 2, pl.ds(tail + members - whole + 1, 1), :] = local


def accumulate(members, chunks, groups, in_refs, start_ref, acc_ref):
    rows, whole = block_rows(members)
    rest = rows - whole
    pad = round_up(rows, 16)
    low_iota = lax.broadcasted_iota(jnp.int32, (WIDE, LANES), 0)
    row_iota = lax.broadcasted_iota(jnp.int32, (pad, LANES), 0)
    blocks = [(ref, b) for ref, picks in in_refs for b in picks]
    for n, (ref, b) in enumerate(blocks):
        parts, lows, highs = [], [], []
        for j in range(chunks):
            tail = whole * chunks + j * rest
            values = jnp.concatenate(
                [
                    ref[b, pl.ds(j * whole, whole), :],
                    ref[b, pl.ds(tail, rest), :],
                    jnp.zeros((pad - rows, LANES), jnp.float32),
                ],
                0,
            )
            cell = ref[b, pl.ds(tail + members - whole + 1, 1), :].astype(jnp.int32)
            live = (cell >= 0).astype(jnp.float32)
            values = jnp.where(row_iota == members + 1, live, values)
            top = values.astype(jnp.bfloat16)
            left_over = values - top.astype(jnp.float32)
            middle = left_over.astype(jnp.bfloat16)
            bottom = (left_over - middle.astype(jnp.float32)).astype(jnp.bfloat16)
            parts.append(jnp.concatenate([top, middle, bottom], 0))
            high = lax.shift_right_arithmetic(cell, 8)
            highs.append(jnp.broadcast_to(high, (3 * pad, LANES)))
            lows.append((low_iota == (cell & (WIDE - 1))).astype(jnp.float32).astype(jnp.bfloat16))
        part = jnp.concatenate(parts, 1)
        high = jnp.concatenate(highs, 1)
        low = jnp.concatenate(lows, 1)
        left = jnp.concatenate(
            [jnp.where(high == g, part, jnp.zeros_like(part)) for g in range(groups)], 0
        )
        product = lax.dot_general(
            left, low, (((1,), (1,)), ((), ())), preferred_element_type=jnp.float32
        )
        if n == 0 and start_ref is None:
            acc_ref[...] = product
        elif n == 0:
            acc_ref[...] = start_ref[...] + product
        else:
            acc_ref[...] += product


def finish(members, groups, acc_ref, dev_ref, moment_ref, error_ref, count_ref):
    pad = round_up(block_rows(members)[0], 16)
    for g in range(groups):
        start, width = g * WIDE, min(WIDE, CELL_DEV - g * WIDE)
        base = g * 3 * pad
        sums = (
            acc_ref[pl.ds(base, pad), :width]
            + acc_ref[pl.ds(base + pad, pad), :width]
            + acc_ref[pl.ds(base + 2 * pad, pad), :width]
        )
        counted = sums[members + 1 : members + 2]
        filled = counted > 0
        total = jnp.where(filled, sums[members : members + 1], 1.0)
        deviation = sums[:members] / total
        moment = jnp.sum(deviation, 0, keepdims=True)
        centred = deviation - moment / members
        spread = jnp.sum(centred * centred, 0, keepdims=True)
        error = jnp.where(filled, 1.0 / total, 0.0)
        count = counted.astype(jnp.int32)
        dev_ref[:, start : start + width] = deviation
        for j in range(width // LANES):
            line, cut = start // LANES + j, slice(j * LANES, (j + 1) * LANES)
            moment_ref[0, line : line + 1, :] = moment[:, cut]
            moment_ref[1, line : line + 1, :] = spread[:, cut]
            error_ref[line : line + 1, :] = error[:, cut]
            count_ref[line : line + 1, :] = count[:, cut]


def near(array):
    return pltpu.with_memory_space_constraint(array, pltpu.VMEM)


def bin_some(members, chunks, arrays, start=None, last=False):
    groups = -(-CELL_DEV // WIDE)
    pad = round_up(block_rows(members)[0], 16)
    lines = CELL_DEV // LANES
    acc = pltpu.VMEM((groups * 3 * pad, WIDE), jnp.float32)
    inputs = [array for array, _ in arrays] + ([] if start is None else [start])

    def body(*refs):
        ins, outs = refs[: len(inputs)], refs[len(inputs) :]
        start_ref = None if start is None else ins[-1]
        pairs = list(zip(ins, [picks for _, picks in arrays]))
        accumulate(members, chunks, groups, pairs, start_ref, outs[-1])
        if last:
            finish(members, groups, outs[-1], *outs[:-1])

    return pl.pallas_call(
        body,
        out_shape=[
            pltpu.VMEM((members, CELL_DEV), jnp.float32),
            pltpu.VMEM((2, lines, LANES), jnp.float32),
            pltpu.VMEM((lines, LANES), jnp.float32),
            pltpu.VMEM((lines, LANES), jnp.int32),
        ]
        if last
        else acc,
        scratch_shapes=[acc] if last else [],
    )(*[near(array) for array in inputs])


def final_kernel(
    total, dev_ref, mine_ref, theirs_ref, error_in, count_in, out_ref, departure_ref, variance_ref, error_ref, count_ref
):
    half = total // 2
    moment = mine_ref[0] + theirs_ref[0]
    gap = mine_ref[0] - theirs_ref[0]
    spread = mine_ref[1] + theirs_ref[1] + gap * gap / (2 * half)
    mean = moment / total
    departure_ref[...] = -mean
    variance_ref[...] = spread / (total - 1)
    error_ref[...] = error_in[...]
    count_ref[...] = count_in[...]
    for j in range(CELL_DEV // LANES):
        cut = slice(j * LANES, (j + 1) * LANES)
        out_ref[:, cut] = dev_ref[:, cut] - mean[j : j + 1]


def merge(mine, theirs, each):
    gap = mine[0] - theirs[0]
    return jnp.stack([mine[0] + theirs[0], mine[1] + theirs[1] + gap * gap / (2 * each)])


def chip_order(chips):
    return list(range(chips - 1, 0, -1))


def step(member_values, obs_value, obs_weight, obs_cell):
    regions = lax.axis_size("reg")
    groups = lax.axis_size("mem")
    members, slots = member_values.shape
    chunks = slots // regions // LANES
    chips = regions // 2
    f32 = functools.partial(jax.ShapeDtypeStruct, dtype=jnp.float32)
    lines = (slots // LANES, LANES)
    same, other = pl.pallas_call(
        functools.partial(pack_kernel, members, regions, chunks),
        out_shape=[pltpu.VMEM((chips, chunks * block_rows(members)[0], LANES), jnp.float32)] * 2,
    )(member_values, obs_value.reshape(lines), obs_weight.reshape(lines), obs_cell.reshape(lines))
    partner = lax.ppermute(other, "reg", [(i, i ^ 1) for i in range(regions)])
    local = [(same, (0,)), (partner, (0,))]
    order = chip_order(chips)
    arrivals = []
    for k in order:
        sent = jnp.stack([same[k], partner[k]])
        arrivals.append((lax.ppermute(sent, "reg", [(i, i ^ (2 * k + 1)) for i in range(regions)]), (0, 1)))
    sums = None
    for n, arrival in enumerate(arrivals):
        sums = bin_some(members, chunks, local * (n == 0) + [arrival], sums, n == chips - 2)
    deviation, moments, error_variance, obs_total = sums
    each, reach = members, 1
    while 2 * reach < groups:
        theirs = lax.ppermute(moments, "mem", [(i, i ^ reach) for i in range(groups)])
        moments = merge(moments, theirs, each)
        each, reach = 2 * each, 2 * reach
    theirs = lax.ppermute(moments, "mem", [(i, i ^ reach) for i in range(groups)])
    cells = (CELL_DEV // LANES, LANES)
    outs = pl.pallas_call(
        functools.partial(final_kernel, members * groups),
        out_shape=[f32((members, CELL_DEV)), f32(cells), f32(cells), f32(cells), jax.ShapeDtypeStruct(cells, jnp.int32)],
    )(*[near(a) for a in (deviation, moments, theirs, error_variance, obs_total)])
    return (outs[0], *[out.reshape(-1) for out in outs[1:]])


def solution(mesh):
    return jax.shard_map(
        step,
        mesh=mesh,
        in_specs=(P("mem", "reg"), P("reg"), P("reg"), P("reg")),
        out_specs=(P("mem", "reg"), P("reg"), P("reg"), P("reg"), P("reg")),
        check_vma=False,
    )
```

```python
import functools
import jax
import jax.numpy as jnp
from jax import lax
from jax.experimental import pallas as pl
from jax.experimental.pallas import tpu as pltpu
from jax.sharding import PartitionSpec as P

CELL_DEV = 1920
LANES = 128
WIDE = 256
LINES = CELL_DEV // LANES
GROUPS = -(-CELL_DEV // WIDE)


def round_up(size, unit):
    return -(-size // unit) * unit


def block_rows(members):
    rows = round_up(members + 2, 4)
    return rows, rows // 8 * 8


def pack_kernel(members, chips, chunks, value_ref, obs_ref, weight_ref, cell_ref, out_ref):
    chip = lax.axis_index("reg") // 2
    rows, whole = block_rows(members)
    rest = rows - whole
    for step in range(chips):
        for core in range(2):
            owner = (chip ^ step) * 2 + core
            for j in range(chunks):
                line = owner * chunks + j
                values = value_ref[:, pl.ds(pl.multiple_of(line * LANES, LANES), LANES)]
                cell = cell_ref[pl.ds(line, 1), :]
                live = cell >= 0
                weight = jnp.where(live, weight_ref[pl.ds(line, 1), :], 0.0)
                local = jnp.where(live, cell - owner * CELL_DEV, -1).astype(jnp.float32)
                innovation = (values - obs_ref[pl.ds(line, 1), :]) * weight
                tail = whole * chunks + j * rest
                out_ref[step, core, pl.ds(j * whole, whole), :] = innovation[:whole]
                out_ref[step, core, pl.ds(tail, members - whole), :] = innovation[whole:]
                out_ref[step, core, pl.ds(tail + members - whole, 1), :] = weight
                out_ref[step, core, pl.ds(tail + members - whole + 1, 1), :] = local


def split(values):
    top = values.astype(jnp.bfloat16).astype(jnp.float32)
    return top, (values - top).astype(jnp.bfloat16).astype(jnp.float32)


def accumulate(members, chunks, in_refs, start_ref, acc_ref):
    rows, whole = block_rows(members)
    rest = rows - whole
    height = GROUPS * 2 * rows
    low_iota = lax.broadcasted_iota(jnp.int32, (WIDE, LANES), 0)
    low_half = low_iota.astype(jnp.float32).astype(jnp.bfloat16)
    one, nil = jnp.ones((), jnp.bfloat16), jnp.zeros((), jnp.bfloat16)
    row_iota = lax.broadcasted_iota(jnp.int32, (2 * rest, LANES), 0)
    blocks = [(core, ref, b) for core in range(2) for ref, picks in in_refs for b in picks]
    seen = set()
    for core, ref, b in blocks:
        pieces, lows = [], []
        for j in range(chunks):
            tail = whole * chunks + j * rest
            main_top, main_rest = split(ref[b, core, pl.ds(j * whole, whole), :])
            end = ref[b, core, pl.ds(tail, rest), :]
            cell = end[members - whole + 1 : members - whole + 2].astype(jnp.int32)
            live = (cell >= 0).astype(jnp.float32)
            end = jnp.concatenate([end, end], 0)
            end = jnp.where(row_iota % rest == members - whole + 1, live, end)
            end_top, end_rest = split(end)
            end = jnp.where(row_iota < rest, end_top, end_rest)
            piece = jnp.concatenate([main_top, main_rest, end], 0)
            high = lax.shift_right_arithmetic(cell, 8)
            pieces.append([jnp.where(high == g, piece, 0.0) for g in range(GROUPS)])
            lows.append(jnp.where(low_half == (cell & (WIDE - 1)).astype(jnp.float32).astype(jnp.bfloat16), one, nil))
        left = jnp.concatenate(
            [jnp.concatenate([p[g] for p in pieces], 1) for g in range(GROUPS)], 0
        ).astype(jnp.bfloat16)
        low = jnp.concatenate(lows, 1)
        product = lax.dot_general(
            left, low, (((1,), (1,)), ((), ())), preferred_element_type=jnp.float32
        )
        spot = pl.ds(core * height, height)
        if core in seen:
            acc_ref[spot, :] += product
        elif start_ref is None:
            acc_ref[spot, :] = product
        else:
            acc_ref[spot, :] = start_ref[spot, :] + product
        seen.add(core)


def finish(members, acc_ref, moment_ref, *result_refs):
    rows, whole = block_rows(members)
    rest, extra = rows - whole, members - whole
    for core, result_ref in enumerate(result_refs):
        for g in range(GROUPS):
            start, width = g * WIDE, min(WIDE, CELL_DEV - g * WIDE)
            base = (core * GROUPS + g) * 2 * rows
            main = acc_ref[pl.ds(base, whole), :width] + acc_ref[pl.ds(base + whole, whole), :width]
            end = acc_ref[pl.ds(base + 2 * whole, 2 * rest), :width]
            end = end[:rest] + end[rest:]
            counted = end[extra + 1 : extra + 2]
            filled = counted > 0
            total = jnp.where(filled, end[extra : extra + 1], 1.0)
            inverse = 1.0 / total
            main = main * inverse
            last = end[:extra] * inverse
            moment = jnp.sum(main, 0, keepdims=True) + jnp.sum(last, 0, keepdims=True)
            mean = moment * (1.0 / members)
            main_gap, last_gap = main - mean, last - mean
            spread = jnp.sum(main_gap * main_gap, 0, keepdims=True) + jnp.sum(last_gap * last_gap, 0, keepdims=True)
            result_ref[:whole, start : start + width] = main
            result_ref[whole:members, start : start + width] = last
            result_ref[members : members + 1, start : start + width] = jnp.where(filled, inverse, 0.0)
            result_ref[members + 1 : members + 2, start : start + width] = counted
            for j in range(width // LANES):
                line, cut = start // LANES + j, slice(j * LANES, (j + 1) * LANES)
                moment_ref[core, 0, line : line + 1, :] = moment[:, cut]
                moment_ref[core, 1, line : line + 1, :] = spread[:, cut]


def near(array):
    return pltpu.with_memory_space_constraint(array, pltpu.VMEM)


def bin_some(members, chunks, arrays, start=None, last=False):
    acc = pltpu.VMEM((2 * GROUPS * 2 * block_rows(members)[0], WIDE), jnp.float32)
    inputs = [array for array, _ in arrays] + ([] if start is None else [start])

    def body(*refs):
        ins, outs = refs[: len(inputs)], refs[len(inputs) :]
        start_ref = None if start is None else ins[-1]
        pairs = list(zip(ins, [picks for _, picks in arrays]))
        accumulate(members, chunks, pairs, start_ref, outs[-1])
        if last:
            finish(members, outs[-1], *outs[:-1])

    return pl.pallas_call(
        body,
        out_shape=[pltpu.VMEM((2, 2, LINES, LANES), jnp.float32)]
        + [pltpu.VMEM((members + 2, CELL_DEV), jnp.float32)] * 2
        if last
        else acc,
        scratch_shapes=[acc] if last else [],
    )(*[near(array) for array in inputs])


def final_kernel(
    members, total, own_ref, passed_ref, moment_ref, far_ref, out_ref, departure_ref, variance_ref, error_ref, count_ref
):
    def write(core, result_ref, merged_ref):
        mean = merged_ref[core, 0] * (1.0 / total)
        departure_ref[...] = -mean
        variance_ref[...] = merged_ref[core, 1] * (1.0 / (total - 1))
        for j in range(LINES):
            cut = slice(j * LANES, (j + 1) * LANES)
            out_ref[:, cut] = result_ref[:members, cut] - mean[j : j + 1]
            error_ref[j : j + 1, :] = result_ref[members : members + 1, cut]
            count_ref[j : j + 1, :] = result_ref[members + 1 : members + 2, cut].astype(jnp.int32)

    core = lax.axis_index("reg") % 2
    pl.when(core == 1)(lambda: write(1, own_ref, moment_ref))
    pl.when(core == 0)(lambda: write(0, passed_ref, far_ref))


def merge(mine, theirs, each):
    gap = mine[:, 0] - theirs[:, 0]
    spread = mine[:, 1] + theirs[:, 1] + gap * gap / (2 * each)
    return jnp.stack([mine[:, 0] + theirs[:, 0], spread], 1)


def chip_order(chips):
    return list(range(chips - 1, 0, -1))


def idle(members, packed, partner):
    shape = (members + 2, CELL_DEV)
    return jnp.zeros((2, 2, LINES, LANES)), jnp.zeros(shape), jnp.zeros(shape)


def hub(members, chunks, regions, packed, partner):
    chips = regions // 2
    arrivals = []
    for k in chip_order(chips):
        sent = jnp.stack([packed[k], partner[k]])
        pairs = [(i, i ^ (2 * k)) for i in range(regions)]
        arrivals.append((lax.ppermute(sent, "reg", pairs), (0, 1)))
    sums = bin_some(members, chunks, [(packed, (0,)), (partner, (0,))])
    for n, arrival in enumerate(arrivals):
        sums = bin_some(members, chunks, [arrival], sums, n == chips - 2)
    return sums


def reduce_mem(members, groups, moments):
    each, reach = members, 1
    while reach < groups:
        theirs = lax.ppermute(moments, "mem", [(z, z ^ reach) for z in range(groups)])
        moments = merge(moments, theirs, each)
        each, reach = 2 * each, 2 * reach
    return moments


def step(member_values, obs_value, obs_weight, obs_cell):
    regions = lax.axis_size("reg")
    groups = lax.axis_size("mem")
    members, slots = member_values.shape
    chunks = slots // regions // LANES
    chips = regions // 2
    swap = [(i, i ^ 1) for i in range(regions)]
    lines = (slots // LANES, LANES)
    packed = pl.pallas_call(
        functools.partial(pack_kernel, members, chips, chunks),
        out_shape=pltpu.VMEM((chips, 2, chunks * block_rows(members)[0], LANES), jnp.float32),
    )(member_values, obs_value.reshape(lines), obs_weight.reshape(lines), obs_cell.reshape(lines))
    partner = lax.ppermute(packed, "reg", swap)
    north = lax.axis_index("reg") % 2 == 1
    moments, passed, own = lax.cond(
        north, functools.partial(hub, members, chunks, regions), functools.partial(idle, members), packed, partner
    )
    passed = lax.ppermute(passed, "reg", swap)
    moments = lax.cond(north, functools.partial(reduce_mem, members, groups), lambda m: m, moments)
    far = lax.ppermute(moments, "reg", swap)
    cells = jax.ShapeDtypeStruct((LINES, LANES), jnp.float32)
    outs = pl.pallas_call(
        functools.partial(final_kernel, members, members * groups),
        out_shape=[
            jax.ShapeDtypeStruct((members, CELL_DEV), jnp.float32),
            cells,
            cells,
            cells,
            jax.ShapeDtypeStruct((LINES, LANES), jnp.int32),
        ],
    )(*[near(a) for a in (own, passed, moments, far)])
    return (outs[0], *[out.reshape(-1) for out in outs[1:]])


def solution(mesh):
    return jax.shard_map(
        step,
        mesh=mesh,
        in_specs=(P("mem", "reg"), P("reg"), P("reg"), P("reg")),
        out_specs=(P("mem", "reg"), P("reg"), P("reg"), P("reg"), P("reg")),
        check_vma=False,
    )
```

```python
import functools
import jax
import jax.numpy as jnp
from jax import lax
from jax.experimental import pallas as pl
from jax.experimental.pallas import tpu as pltpu
from jax.sharding import PartitionSpec as P

CELL_DEV = 1920
LANES = 128
WIDE = 256
LINES = CELL_DEV // LANES
GROUPS = -(-CELL_DEV // WIDE)


def round_up(size, unit):
    return -(-size // unit) * unit


def block_rows(members):
    rows = round_up(members + 2, 4)
    return rows, rows // 8 * 8


def odd_plane():
    plane = lax.axis_index("mem")
    odd = plane & 1
    for bit in range(1, lax.axis_size("mem").bit_length() - 1):
        odd = odd ^ (lax.shift_right_logical(plane, bit) & 1)
    return odd


def pack_kernel(members, regions, chunks, value_ref, obs_ref, weight_ref, cell_ref, same_ref, other_ref):
    me, odd = lax.axis_index("reg"), odd_plane()
    rows, whole = block_rows(members)
    rest = rows - whole
    for step in range(regions):
        owner = me ^ step ^ odd
        out_ref = other_ref if (step % 2) ^ (step > 1) else same_ref
        for j in range(chunks):
            line = owner * chunks + j
            values = value_ref[:, pl.ds(pl.multiple_of(line * LANES, LANES), LANES)]
            cell = cell_ref[pl.ds(line, 1), :]
            live = cell >= 0
            weight = jnp.where(live, weight_ref[pl.ds(line, 1), :], 0.0)
            local = jnp.where(live, cell - owner * CELL_DEV, -1).astype(jnp.float32)
            innovation = (values - obs_ref[pl.ds(line, 1), :]) * weight
            tail = whole * chunks + j * rest
            out_ref[step // 2, pl.ds(j * whole, whole), :] = innovation[:whole]
            out_ref[step // 2, pl.ds(tail, members - whole), :] = innovation[whole:]
            out_ref[step // 2, pl.ds(tail + members - whole, 1), :] = weight
            out_ref[step // 2, pl.ds(tail + members - whole + 1, 1), :] = local


def split(values):
    top = values.astype(jnp.bfloat16).astype(jnp.float32)
    return top, (values - top).astype(jnp.bfloat16).astype(jnp.float32)


def accumulate(members, chunks, in_refs, start_ref, acc_ref):
    rows, whole = block_rows(members)
    rest = rows - whole
    low_iota = lax.broadcasted_iota(jnp.int32, (WIDE, LANES), 0)
    low_half = low_iota.astype(jnp.float32).astype(jnp.bfloat16)
    one, nil = jnp.ones((), jnp.bfloat16), jnp.zeros((), jnp.bfloat16)
    row_iota = lax.broadcasted_iota(jnp.int32, (2 * rest, LANES), 0)
    blocks = [(ref, b) for ref, picks in in_refs for b in picks]
    for n, (ref, b) in enumerate(blocks):
        pieces, lows = [], []
        for j in range(chunks):
            tail = whole * chunks + j * rest
            main_top, main_rest = split(ref[b, pl.ds(j * whole, whole), :])
            end = ref[b, pl.ds(tail, rest), :]
            cell = end[members - whole + 1 : members - whole + 2].astype(jnp.int32)
            live = (cell >= 0).astype(jnp.float32)
            end = jnp.concatenate([end, end], 0)
            end = jnp.where(row_iota % rest == members - whole + 1, live, end)
            end_top, end_rest = split(end)
            end = jnp.where(row_iota < rest, end_top, end_rest)
            piece = jnp.concatenate([main_top, main_rest, end], 0)
            high = lax.shift_right_arithmetic(cell, 8)
            pieces.append([jnp.where(high == g, piece, 0.0) for g in range(GROUPS)])
            lows.append(jnp.where(low_half == (cell & (WIDE - 1)).astype(jnp.float32).astype(jnp.bfloat16), one, nil))
        left = jnp.concatenate(
            [jnp.concatenate([p[g] for p in pieces], 1) for g in range(GROUPS)], 0
        ).astype(jnp.bfloat16)
        low = jnp.concatenate(lows, 1)
        product = lax.dot_general(
            left, low, (((1,), (1,)), ((), ())), preferred_element_type=jnp.float32
        )
        if n:
            acc_ref[...] += product
        elif start_ref is None:
            acc_ref[...] = product
        else:
            acc_ref[...] = start_ref[...] + product


def finish(members, acc_ref, moment_ref, result_ref):
    rows, whole = block_rows(members)
    rest, extra = rows - whole, members - whole
    for g in range(GROUPS):
        start, width = g * WIDE, min(WIDE, CELL_DEV - g * WIDE)
        base = g * 2 * rows
        main = acc_ref[pl.ds(base, whole), :width] + acc_ref[pl.ds(base + whole, whole), :width]
        end = acc_ref[pl.ds(base + 2 * whole, 2 * rest), :width]
        end = end[:rest] + end[rest:]
        counted = end[extra + 1 : extra + 2]
        filled = counted > 0
        total = jnp.where(filled, end[extra : extra + 1], 1.0)
        inverse = 1.0 / total
        main = main * inverse
        last = end[:extra] * inverse
        moment = jnp.sum(main, 0, keepdims=True) + jnp.sum(last, 0, keepdims=True)
        mean = moment * (1.0 / members)
        main_gap, last_gap = main - mean, last - mean
        spread = jnp.sum(main_gap * main_gap, 0, keepdims=True) + jnp.sum(last_gap * last_gap, 0, keepdims=True)
        error = jnp.where(filled, inverse, 0.0)
        for j in range(width // LANES):
            line, cut = start // LANES + j, slice(j * LANES, (j + 1) * LANES)
            tail = LINES * whole + line * rest
            result_ref[line * whole : (line + 1) * whole, :] = main[:, cut]
            result_ref[tail : tail + extra, :] = last[:, cut]
            result_ref[tail + extra : tail + extra + 1, :] = error[:, cut]
            result_ref[tail + extra + 1 : tail + extra + 2, :] = counted[:, cut]
            moment_ref[0, line : line + 1, :] = moment[:, cut]
            moment_ref[1, line : line + 1, :] = spread[:, cut]


def near(array):
    return pltpu.with_memory_space_constraint(array, pltpu.VMEM)


def bin_some(members, chunks, arrays, start=None, last=False):
    acc = pltpu.VMEM((GROUPS * 2 * block_rows(members)[0], WIDE), jnp.float32)
    inputs = [array for array, _ in arrays] + ([] if start is None else [start])

    def body(*refs):
        ins, outs = refs[: len(inputs)], refs[len(inputs) :]
        start_ref = None if start is None else ins[-1]
        pairs = list(zip(ins, [picks for _, picks in arrays]))
        accumulate(members, chunks, pairs, start_ref, outs[-1])
        if last:
            finish(members, outs[-1], *outs[:-1])

    return pl.pallas_call(
        body,
        out_shape=[
            pltpu.VMEM((2, LINES, LANES), jnp.float32),
            pltpu.VMEM((LINES * block_rows(members)[0], LANES), jnp.float32),
        ]
        if last
        else acc,
        scratch_shapes=[acc] if last else [],
    )(*[near(array) for array in inputs])


def final_kernel(
    members, total, own_ref, passed_ref, moment_ref, out_ref, departure_ref, variance_ref, error_ref, count_ref
):
    mean = moment_ref[0] * (1.0 / total)
    departure_ref[...] = -mean
    variance_ref[...] = moment_ref[1] * (1.0 / (total - 1))

    rows, whole = block_rows(members)
    rest, extra = rows - whole, members - whole

    def write(result_ref):
        for j in range(LINES):
            cut = slice(j * LANES, (j + 1) * LANES)
            tail = LINES * whole + j * rest
            line, below = mean[j : j + 1], slice(tail + extra, tail + extra + 1)
            out_ref[:whole, cut] = result_ref[j * whole : (j + 1) * whole, :] - line
            out_ref[whole:, cut] = result_ref[tail : tail + extra, :] - line
            error_ref[j : j + 1, :] = result_ref[below, :]
            count_ref[j : j + 1, :] = result_ref[tail + extra + 1 : tail + extra + 2, :].astype(jnp.int32)

    odd = odd_plane()
    pl.when(odd == 0)(lambda: write(own_ref))
    pl.when(odd == 1)(lambda: write(passed_ref))


def merge(mine, theirs, each):
    gap = mine[0] - theirs[0]
    return jnp.stack([mine[0] + theirs[0], mine[1] + theirs[1] + gap * gap / (2 * each)])


def chip_order(chips):
    return list(range(chips - 1, 0, -1))


def step(member_values, obs_value, obs_weight, obs_cell):
    regions = lax.axis_size("reg")
    groups = lax.axis_size("mem")
    members, slots = member_values.shape
    chunks = slots // regions // LANES
    chips = regions // 2
    swap = [(i, i ^ 1) for i in range(regions)]
    lines = (slots // LANES, LANES)
    same, other = pl.pallas_call(
        functools.partial(pack_kernel, members, regions, chunks),
        out_shape=[pltpu.VMEM((chips, chunks * block_rows(members)[0], LANES), jnp.float32)] * 2,
    )(member_values, obs_value.reshape(lines), obs_weight.reshape(lines), obs_cell.reshape(lines))
    partner = lax.ppermute(other, "reg", swap)
    arrivals = []
    for k in chip_order(chips):
        sent = jnp.stack([same[k], partner[k]])
        pairs = [(i, i ^ (2 * k + 1)) for i in range(regions)]
        arrivals.append((lax.ppermute(sent, "reg", pairs), (0, 1)))
    sums = bin_some(members, chunks, [(same, (0,)), (partner, (0,))])
    for n, arrival in enumerate(arrivals):
        sums = bin_some(members, chunks, [arrival], sums, n == chips - 2)
    moments, own = sums
    passed = lax.ppermute(own, "reg", swap)
    each, reach = members, 1
    while reach < groups:
        pairs = [(z * regions + i, (z ^ reach) * regions + (i ^ 1)) for z in range(groups) for i in range(regions)]
        theirs = lax.ppermute(moments, ("mem", "reg"), pairs)
        moments = merge(moments, theirs, each)
        each, reach = 2 * each, 2 * reach
    moments = lax.cond(odd_plane() == 1, lambda m: lax.ppermute(m, "reg", swap), lambda m: m, moments)
    cells = jax.ShapeDtypeStruct((LINES, LANES), jnp.float32)
    outs = pl.pallas_call(
        functools.partial(final_kernel, members, members * groups),
        out_shape=[
            jax.ShapeDtypeStruct((members, CELL_DEV), jnp.float32),
            cells,
            cells,
            cells,
            jax.ShapeDtypeStruct((LINES, LANES), jnp.int32),
        ],
    )(*[near(a) for a in (own, passed, moments)])
    return (outs[0], *[out.reshape(-1) for out in outs[1:]])


def solution(mesh):
    return jax.shard_map(
        step,
        mesh=mesh,
        in_specs=(P("mem", "reg"), P("reg"), P("reg"), P("reg")),
        out_specs=(P("mem", "reg"), P("reg"), P("reg"), P("reg"), P("reg")),
        check_vma=False,
    )
```

```python
import functools
import jax
import jax.numpy as jnp
from jax import lax
from jax.experimental import pallas as pl
from jax.experimental.pallas import tpu as pltpu
from jax.sharding import PartitionSpec as P

CELL_DEV = 1920
LANES = 128
WIDE = 256
LINES = CELL_DEV // LANES
GROUPS = -(-CELL_DEV // WIDE)


def round_up(size, unit):
    return -(-size // unit) * unit


def block_rows(members):
    rows = round_up(members + 2, 4)
    return rows, rows // 8 * 8


def odd_plane():
    plane = lax.axis_index("mem")
    odd = plane & 1
    for bit in range(1, lax.axis_size("mem").bit_length() - 1):
        odd = odd ^ (lax.shift_right_logical(plane, bit) & 1)
    return odd


def pack_kernel(members, regions, chunks, value_ref, obs_ref, weight_ref, cell_ref, same_ref, other_ref, direct_ref):
    me, odd = lax.axis_index("reg"), odd_plane()
    rows, whole = block_rows(members)
    rest = rows - whole
    for step in range(regions):
        owner = me ^ step ^ odd
        if step // 2 == regions // 2 - 1:
            out_ref, slot = direct_ref, 1 - step % 2
        else:
            out_ref, slot = other_ref if (step % 2) ^ (step > 1) else same_ref, step // 2
        for j in range(chunks):
            line = owner * chunks + j
            values = value_ref[:, pl.ds(pl.multiple_of(line * LANES, LANES), LANES)]
            cell = cell_ref[pl.ds(line, 1), :]
            live = cell >= 0
            weight = jnp.where(live, weight_ref[pl.ds(line, 1), :], 0.0)
            local = jnp.where(live, cell - owner * CELL_DEV, -1).astype(jnp.float32)
            innovation = (values - obs_ref[pl.ds(line, 1), :]) * weight
            tail = whole * chunks + j * rest
            out_ref[slot, pl.ds(j * whole, whole), :] = innovation[:whole]
            out_ref[slot, pl.ds(tail, members - whole), :] = innovation[whole:]
            out_ref[slot, pl.ds(tail + members - whole, 1), :] = weight
            out_ref[slot, pl.ds(tail + members - whole + 1, 1), :] = local


def split(values):
    top = values.astype(jnp.bfloat16).astype(jnp.float32)
    return top, (values - top).astype(jnp.bfloat16).astype(jnp.float32)


def accumulate(members, chunks, in_refs, start_ref, acc_ref):
    rows, whole = block_rows(members)
    rest = rows - whole
    low_iota = lax.broadcasted_iota(jnp.int32, (WIDE, LANES), 0)
    low_half = low_iota.astype(jnp.float32).astype(jnp.bfloat16)
    one, nil = jnp.ones((), jnp.bfloat16), jnp.zeros((), jnp.bfloat16)
    row_iota = lax.broadcasted_iota(jnp.int32, (2 * rest, LANES), 0)
    blocks = [(ref, b) for ref, picks in in_refs for b in picks]
    for n, (ref, b) in enumerate(blocks):
        pieces, lows = [], []
        for j in range(chunks):
            tail = whole * chunks + j * rest
            main_top, main_rest = split(ref[b, pl.ds(j * whole, whole), :])
            end = ref[b, pl.ds(tail, rest), :]
            cell = end[members - whole + 1 : members - whole + 2].astype(jnp.int32)
            live = (cell >= 0).astype(jnp.float32)
            end = jnp.concatenate([end, end], 0)
            end = jnp.where(row_iota % rest == members - whole + 1, live, end)
            end_top, end_rest = split(end)
            end = jnp.where(row_iota < rest, end_top, end_rest)
            piece = jnp.concatenate([main_top, main_rest, end], 0)
            high = lax.shift_right_arithmetic(cell, 8)
            pieces.append([jnp.where(high == g, piece, 0.0) for g in range(GROUPS)])
            lows.append(jnp.where(low_half == (cell & (WIDE - 1)).astype(jnp.float32).astype(jnp.bfloat16), one, nil))
        left = jnp.concatenate(
            [jnp.concatenate([p[g] for p in pieces], 1) for g in range(GROUPS)], 0
        ).astype(jnp.bfloat16)
        low = jnp.concatenate(lows, 1)
        product = lax.dot_general(
            left, low, (((1,), (1,)), ((), ())), preferred_element_type=jnp.float32
        )
        if n:
            acc_ref[...] += product
        elif start_ref is None:
            acc_ref[...] = product
        else:
            acc_ref[...] = start_ref[...] + product


def finish(members, acc_ref, moment_ref, result_ref):
    rows, whole = block_rows(members)
    rest, extra = rows - whole, members - whole
    for g in range(GROUPS):
        start, width = g * WIDE, min(WIDE, CELL_DEV - g * WIDE)
        base = g * 2 * rows
        main = acc_ref[pl.ds(base, whole), :width] + acc_ref[pl.ds(base + whole, whole), :width]
        end = acc_ref[pl.ds(base + 2 * whole, 2 * rest), :width]
        end = end[:rest] + end[rest:]
        counted = end[extra + 1 : extra + 2]
        filled = counted > 0
        total = jnp.where(filled, end[extra : extra + 1], 1.0)
        inverse = 1.0 / total
        main = main * inverse
        last = end[:extra] * inverse
        moment = jnp.sum(main, 0, keepdims=True) + jnp.sum(last, 0, keepdims=True)
        mean = moment * (1.0 / members)
        main_gap, last_gap = main - mean, last - mean
        spread = jnp.sum(main_gap * main_gap, 0, keepdims=True) + jnp.sum(last_gap * last_gap, 0, keepdims=True)
        error = jnp.where(filled, inverse, 0.0)
        for j in range(width // LANES):
            line, cut = start // LANES + j, slice(j * LANES, (j + 1) * LANES)
            tail = LINES * whole + line * rest
            result_ref[line * whole : (line + 1) * whole, :] = main[:, cut]
            result_ref[tail : tail + extra, :] = last[:, cut]
            result_ref[tail + extra : tail + extra + 1, :] = error[:, cut]
            result_ref[tail + extra + 1 : tail + extra + 2, :] = counted[:, cut]
            moment_ref[0, line : line + 1, :] = moment[:, cut]
            moment_ref[1, line : line + 1, :] = spread[:, cut]


def near(array):
    return pltpu.with_memory_space_constraint(array, pltpu.VMEM)


def bin_some(members, chunks, arrays, start=None, last=False):
    acc = pltpu.VMEM((GROUPS * 2 * block_rows(members)[0], WIDE), jnp.float32)
    inputs = [array for array, _ in arrays] + ([] if start is None else [start])

    def body(*refs):
        ins, outs = refs[: len(inputs)], refs[len(inputs) :]
        start_ref = None if start is None else ins[-1]
        pairs = list(zip(ins, [picks for _, picks in arrays]))
        accumulate(members, chunks, pairs, start_ref, outs[-1])
        if last:
            finish(members, outs[-1], *outs[:-1])

    return pl.pallas_call(
        body,
        out_shape=[
            pltpu.VMEM((2, LINES, LANES), jnp.float32),
            pltpu.VMEM((LINES * block_rows(members)[0], LANES), jnp.float32),
        ]
        if last
        else acc,
        scratch_shapes=[acc] if last else [],
    )(*[near(array) for array in inputs])


def final_kernel(
    members, total, own_ref, passed_ref, moment_ref, out_ref, departure_ref, variance_ref, error_ref, count_ref
):
    mean = moment_ref[0] * (1.0 / total)
    departure_ref[...] = -mean
    variance_ref[...] = moment_ref[1] * (1.0 / (total - 1))

    rows, whole = block_rows(members)
    rest, extra = rows - whole, members - whole

    def write(result_ref):
        for j in range(LINES):
            cut = slice(j * LANES, (j + 1) * LANES)
            tail = LINES * whole + j * rest
            line, below = mean[j : j + 1], slice(tail + extra, tail + extra + 1)
            out_ref[:whole, cut] = result_ref[j * whole : (j + 1) * whole, :] - line
            out_ref[whole:, cut] = result_ref[tail : tail + extra, :] - line
            error_ref[j : j + 1, :] = result_ref[below, :]
            count_ref[j : j + 1, :] = result_ref[tail + extra + 1 : tail + extra + 2, :].astype(jnp.int32)

    odd = odd_plane()
    pl.when(odd == 0)(lambda: write(own_ref))
    pl.when(odd == 1)(lambda: write(passed_ref))


def merge(mine, theirs, each):
    gap = mine[0] - theirs[0]
    return jnp.stack([mine[0] + theirs[0], mine[1] + theirs[1] + gap * gap / (2 * each)])


def chip_order(chips):
    return list(range(chips - 1, 0, -1))


def step(member_values, obs_value, obs_weight, obs_cell):
    regions = lax.axis_size("reg")
    groups = lax.axis_size("mem")
    members, slots = member_values.shape
    chunks = slots // regions // LANES
    chips = regions // 2
    swap = [(i, i ^ 1) for i in range(regions)]
    lines = (slots // LANES, LANES)
    shape = (chunks * block_rows(members)[0], LANES)
    same, other, direct = pl.pallas_call(
        functools.partial(pack_kernel, members, regions, chunks),
        out_shape=[pltpu.VMEM((n, *shape), jnp.float32) for n in (chips - 1, chips - 1, 2)],
    )(member_values, obs_value.reshape(lines), obs_weight.reshape(lines), obs_cell.reshape(lines))
    partner = lax.ppermute(other, "reg", swap)
    arrivals = []
    for k in chip_order(chips):
        sent = direct if k == chips - 1 else jnp.stack([same[k], partner[k]])
        pairs = [(i, i ^ (2 * k + 1)) for i in range(regions)]
        arrivals.append((lax.ppermute(sent, "reg", pairs), (0, 1)))
    landed = arrivals[0][0]
    forwarded = (lax.ppermute(landed, "reg", swap), (1,))
    sums = bin_some(members, chunks, [(same, (0,)), (partner, (0,))])
    for n, arrival in enumerate(arrivals):
        taken = [(landed, (0,))] if n == 0 else [arrival, forwarded] if n == 2 else [arrival]
        sums = bin_some(members, chunks, taken, sums, n == chips - 2)
    moments, own = sums
    passed = lax.ppermute(own, "reg", swap)
    each, reach = members, 1
    while reach < groups:
        pairs = [(z * regions + i, (z ^ reach) * regions + (i ^ 1)) for z in range(groups) for i in range(regions)]
        theirs = lax.ppermute(moments, ("mem", "reg"), pairs)
        moments = merge(moments, theirs, each)
        each, reach = 2 * each, 2 * reach
    moments = lax.cond(odd_plane() == 1, lambda m: lax.ppermute(m, "reg", swap), lambda m: m, moments)
    cells = jax.ShapeDtypeStruct((LINES, LANES), jnp.float32)
    outs = pl.pallas_call(
        functools.partial(final_kernel, members, members * groups),
        out_shape=[
            jax.ShapeDtypeStruct((members, CELL_DEV), jnp.float32),
            cells,
            cells,
            cells,
            jax.ShapeDtypeStruct((LINES, LANES), jnp.int32),
        ],
    )(*[near(a) for a in (own, passed, moments)])
    return (outs[0], *[out.reshape(-1) for out in outs[1:]])


def solution(mesh):
    return jax.shard_map(
        step,
        mesh=mesh,
        in_specs=(P("mem", "reg"), P("reg"), P("reg"), P("reg")),
        out_specs=(P("mem", "reg"), P("reg"), P("reg"), P("reg"), P("reg")),
        check_vma=False,
    )
```

```python
import functools
import jax
import jax.numpy as jnp
from jax import lax
from jax.experimental import pallas as pl
from jax.experimental.pallas import tpu as pltpu
from jax.sharding import PartitionSpec as P

CELL_DEV = 1920
LANES = 128
WIDE = 256
LINES = CELL_DEV // LANES
GROUPS = -(-CELL_DEV // WIDE)


def round_up(size, unit):
    return -(-size // unit) * unit


def block_rows(members):
    rows = round_up(members + 2, 4)
    return rows, rows // 8 * 8


def odd_plane():
    plane = lax.axis_index("mem")
    odd = plane & 1
    for bit in range(1, lax.axis_size("mem").bit_length() - 1):
        odd = odd ^ (lax.shift_right_logical(plane, bit) & 1)
    return odd


def pack_kernel(members, regions, chunks, value_ref, obs_ref, weight_ref, cell_ref, same_ref, other_ref, direct_ref):
    me, odd = lax.axis_index("reg"), odd_plane()
    rows, whole = block_rows(members)
    rest = rows - whole
    for step in range(regions):
        owner = me ^ step ^ odd
        if step // 2 == regions // 2 - 1:
            out_ref, slot = direct_ref, 1 - step % 2
        else:
            out_ref, slot = other_ref if (step % 2) ^ (step > 1) else same_ref, step // 2
        for j in range(chunks):
            line = owner * chunks + j
            values = value_ref[:, pl.ds(pl.multiple_of(line * LANES, LANES), LANES)]
            cell = cell_ref[pl.ds(line, 1), :]
            live = cell >= 0
            weight = jnp.where(live, weight_ref[pl.ds(line, 1), :], 0.0)
            local = jnp.where(live, cell - owner * CELL_DEV, -1).astype(jnp.float32)
            innovation = (values - obs_ref[pl.ds(line, 1), :]) * weight
            tail = whole * chunks + j * rest
            out_ref[slot, pl.ds(j * whole, whole), :] = innovation[:whole]
            out_ref[slot, pl.ds(tail, members - whole), :] = innovation[whole:]
            out_ref[slot, pl.ds(tail + members - whole, 1), :] = weight
            out_ref[slot, pl.ds(tail + members - whole + 1, 1), :] = local


def split(values):
    top = values.astype(jnp.bfloat16).astype(jnp.float32)
    return top, (values - top).astype(jnp.bfloat16).astype(jnp.float32)


def accumulate(members, chunks, in_refs, start_ref, acc_ref):
    rows, whole = block_rows(members)
    rest = rows - whole
    low_iota = lax.broadcasted_iota(jnp.int32, (WIDE, LANES), 0)
    low_half = low_iota.astype(jnp.float32).astype(jnp.bfloat16)
    one, nil = jnp.ones((), jnp.bfloat16), jnp.zeros((), jnp.bfloat16)
    row_iota = lax.broadcasted_iota(jnp.int32, (2 * rest, LANES), 0)
    blocks = [(ref, b) for ref, picks in in_refs for b in picks]
    for n, (ref, b) in enumerate(blocks):
        pieces, lows = [], []
        for j in range(chunks):
            tail = whole * chunks + j * rest
            main_top, main_rest = split(ref[b, pl.ds(j * whole, whole), :])
            end = ref[b, pl.ds(tail, rest), :]
            cell = end[members - whole + 1 : members - whole + 2].astype(jnp.int32)
            live = (cell >= 0).astype(jnp.float32)
            end = jnp.concatenate([end, end], 0)
            end = jnp.where(row_iota % rest == members - whole + 1, live, end)
            end_top, end_rest = split(end)
            end = jnp.where(row_iota < rest, end_top, end_rest)
            piece = jnp.concatenate([main_top, main_rest, end], 0)
            high = lax.shift_right_arithmetic(cell, 8)
            pieces.append([jnp.where(high == g, piece, 0.0) for g in range(GROUPS)])
            lows.append(jnp.where(low_half == (cell & (WIDE - 1)).astype(jnp.float32).astype(jnp.bfloat16), one, nil))
        left = jnp.concatenate(
            [jnp.concatenate([p[g] for p in pieces], 1) for g in range(GROUPS)], 0
        ).astype(jnp.bfloat16)
        low = jnp.concatenate(lows, 1)
        product = lax.dot_general(
            left, low, (((1,), (1,)), ((), ())), preferred_element_type=jnp.float32
        )
        if n:
            acc_ref[...] += product
        elif start_ref is None:
            acc_ref[...] = product
        else:
            acc_ref[...] = start_ref[...] + product


def finish(members, acc_ref, moment_ref, result_ref):
    rows, whole = block_rows(members)
    rest, extra = rows - whole, members - whole
    for g in range(GROUPS):
        start, width = g * WIDE, min(WIDE, CELL_DEV - g * WIDE)
        base = g * 2 * rows
        main = acc_ref[pl.ds(base, whole), :width] + acc_ref[pl.ds(base + whole, whole), :width]
        end = acc_ref[pl.ds(base + 2 * whole, 2 * rest), :width]
        end = end[:rest] + end[rest:]
        counted = end[extra + 1 : extra + 2]
        filled = counted > 0
        total = jnp.where(filled, end[extra : extra + 1], 1.0)
        inverse = 1.0 / total
        main = main * inverse
        last = end[:extra] * inverse
        moment = jnp.sum(main, 0, keepdims=True) + jnp.sum(last, 0, keepdims=True)
        mean = moment * (1.0 / members)
        main_gap, last_gap = main - mean, last - mean
        spread = jnp.sum(main_gap * main_gap, 0, keepdims=True) + jnp.sum(last_gap * last_gap, 0, keepdims=True)
        error = jnp.where(filled, inverse, 0.0)
        for j in range(width // LANES):
            line, cut = start // LANES + j, slice(j * LANES, (j + 1) * LANES)
            tail = LINES * whole + line * rest
            result_ref[line * whole : (line + 1) * whole, :] = main[:, cut]
            result_ref[tail : tail + extra, :] = last[:, cut]
            result_ref[tail + extra : tail + extra + 1, :] = error[:, cut]
            result_ref[tail + extra + 1 : tail + extra + 2, :] = counted[:, cut]
            moment_ref[0, line : line + 1, :] = moment[:, cut]
            moment_ref[1, line : line + 1, :] = spread[:, cut]


def near(array):
    return pltpu.with_memory_space_constraint(array, pltpu.VMEM)


def bin_some(members, chunks, arrays, start=None, last=False):
    acc = pltpu.VMEM((GROUPS * 2 * block_rows(members)[0], WIDE), jnp.float32)
    inputs = [array for array, _ in arrays] + ([] if start is None else [start])

    def body(*refs):
        ins, outs = refs[: len(inputs)], refs[len(inputs) :]
        start_ref = None if start is None else ins[-1]
        pairs = list(zip(ins, [picks for _, picks in arrays]))
        accumulate(members, chunks, pairs, start_ref, outs[-1])
        if last:
            finish(members, outs[-1], *outs[:-1])

    return pl.pallas_call(
        body,
        out_shape=[
            pltpu.VMEM((2, LINES, LANES), jnp.float32),
            pltpu.VMEM((LINES * block_rows(members)[0], LANES), jnp.float32),
        ]
        if last
        else acc,
        scratch_shapes=[acc] if last else [],
    )(*[near(array) for array in inputs])


def final_kernel(
    members, total, own_ref, passed_ref, moment_ref, out_ref, departure_ref, variance_ref, error_ref, count_ref
):
    mean = moment_ref[0] * (1.0 / total)
    departure_ref[...] = -mean
    variance_ref[...] = moment_ref[1] * (1.0 / (total - 1))

    rows, whole = block_rows(members)
    rest, extra = rows - whole, members - whole

    def write(result_ref):
        for j in range(LINES):
            cut = slice(j * LANES, (j + 1) * LANES)
            tail = LINES * whole + j * rest
            line, below = mean[j : j + 1], slice(tail + extra, tail + extra + 1)
            out_ref[:whole, cut] = result_ref[j * whole : (j + 1) * whole, :] - line
            out_ref[whole:, cut] = result_ref[tail : tail + extra, :] - line
            error_ref[j : j + 1, :] = result_ref[below, :]
            count_ref[j : j + 1, :] = result_ref[tail + extra + 1 : tail + extra + 2, :].astype(jnp.int32)

    odd = odd_plane()
    pl.when(odd == 0)(lambda: write(own_ref))
    pl.when(odd == 1)(lambda: write(passed_ref))


def merge(mine, theirs, each):
    gap = mine[0] - theirs[0]
    return jnp.stack([mine[0] + theirs[0], mine[1] + theirs[1] + gap * gap / (2 * each)])


def chip_order(chips):
    return list(range(chips - 1, 0, -1))


def step(member_values, obs_value, obs_weight, obs_cell):
    regions = lax.axis_size("reg")
    groups = lax.axis_size("mem")
    members, slots = member_values.shape
    chunks = slots // regions // LANES
    chips = regions // 2
    swap = [(i, i ^ 1) for i in range(regions)]
    lines = (slots // LANES, LANES)
    shape = (chunks * block_rows(members)[0], LANES)
    same, other, direct = pl.pallas_call(
        functools.partial(pack_kernel, members, regions, chunks),
        out_shape=[pltpu.VMEM((n, *shape), jnp.float32) for n in (chips - 1, chips - 1, 2)],
    )(member_values, obs_value.reshape(lines), obs_weight.reshape(lines), obs_cell.reshape(lines))
    partner = lax.ppermute(other, "reg", swap)
    arrivals = []
    for k in chip_order(chips):
        sent = direct if k == chips - 1 else jnp.stack([same[k], partner[k]])
        pairs = [(i, i ^ (2 * k + 1)) for i in range(regions)]
        arrivals.append((lax.ppermute(sent, "reg", pairs), (0, 1)))
    landed = arrivals[0][0]
    forwarded = (lax.ppermute(landed, "reg", swap), (1,))
    sums = bin_some(members, chunks, [(same, (0,)), (partner, (0,))])
    sums = bin_some(members, chunks, [(landed, (0,))], sums)
    sums = bin_some(members, chunks, [forwarded], sums)
    sums = bin_some(members, chunks, arrivals[1:], sums, True)
    moments, own = sums
    passed = lax.ppermute(own, "reg", swap)
    each, reach = members, 1
    while reach < groups:
        pairs = [(z * regions + i, (z ^ reach) * regions + (i ^ 1)) for z in range(groups) for i in range(regions)]
        theirs = lax.ppermute(moments, ("mem", "reg"), pairs)
        moments = merge(moments, theirs, each)
        each, reach = 2 * each, 2 * reach
    moments = lax.cond(odd_plane() == 1, lambda m: lax.ppermute(m, "reg", swap), lambda m: m, moments)
    cells = jax.ShapeDtypeStruct((LINES, LANES), jnp.float32)
    outs = pl.pallas_call(
        functools.partial(final_kernel, members, members * groups),
        out_shape=[
            jax.ShapeDtypeStruct((members, CELL_DEV), jnp.float32),
            cells,
            cells,
            cells,
            jax.ShapeDtypeStruct((LINES, LANES), jnp.int32),
        ],
    )(*[near(a) for a in (own, passed, moments)])
    return (outs[0], *[out.reshape(-1) for out in outs[1:]])


def solution(mesh):
    return jax.shard_map(
        step,
        mesh=mesh,
        in_specs=(P("mem", "reg"), P("reg"), P("reg"), P("reg")),
        out_specs=(P("mem", "reg"), P("reg"), P("reg"), P("reg"), P("reg")),
        check_vma=False,
    )
```

```python
import functools
import jax
import jax.numpy as jnp
from jax import lax
from jax.experimental import pallas as pl
from jax.experimental.pallas import tpu as pltpu
from jax.sharding import PartitionSpec as P

CELL_DEV = 1920
LANES = 128
WIDE = 256
LINES = CELL_DEV // LANES
GROUPS = -(-CELL_DEV // WIDE)


def round_up(size, unit):
    return -(-size // unit) * unit


def block_rows(members):
    rows = round_up(members + 2, 4)
    return rows, rows // 8 * 8


def odd_plane():
    plane = lax.axis_index("mem")
    odd = plane & 1
    for bit in range(1, lax.axis_size("mem").bit_length() - 1):
        odd = odd ^ (lax.shift_right_logical(plane, bit) & 1)
    return odd


def pack_kernel(members, regions, chunks, value_ref, obs_ref, weight_ref, cell_ref, same_ref, other_ref, direct_ref):
    me, odd = lax.axis_index("reg"), odd_plane()
    rows, whole = block_rows(members)
    rest = rows - whole
    for step in range(regions):
        owner = me ^ step ^ odd
        if step // 2 == regions // 2 - 1:
            out_ref, slot = direct_ref, 1 - step % 2
        else:
            out_ref, slot = other_ref if (step % 2) ^ (step > 1) else same_ref, step // 2
        for j in range(chunks):
            line = owner * chunks + j
            values = value_ref[:, pl.ds(pl.multiple_of(line * LANES, LANES), LANES)]
            cell = cell_ref[pl.ds(line, 1), :]
            live = cell >= 0
            weight = jnp.where(live, weight_ref[pl.ds(line, 1), :], 0.0)
            local = jnp.where(live, cell - owner * CELL_DEV, -1).astype(jnp.float32)
            innovation = (values - obs_ref[pl.ds(line, 1), :]) * weight
            tail = whole * chunks + j * rest
            out_ref[slot, pl.ds(j * whole, whole), :] = innovation[:whole]
            out_ref[slot, pl.ds(tail, members - whole), :] = innovation[whole:]
            out_ref[slot, pl.ds(tail + members - whole, 1), :] = weight
            out_ref[slot, pl.ds(tail + members - whole + 1, 1), :] = local


def split(values):
    top = values.astype(jnp.bfloat16).astype(jnp.float32)
    return top, (values - top).astype(jnp.bfloat16).astype(jnp.float32)


def accumulate(members, chunks, in_refs, start_ref, acc_ref):
    rows, whole = block_rows(members)
    rest = rows - whole
    low_iota = lax.broadcasted_iota(jnp.int32, (WIDE, LANES), 0)
    low_half = low_iota.astype(jnp.float32).astype(jnp.bfloat16)
    one, nil = jnp.ones((), jnp.bfloat16), jnp.zeros((), jnp.bfloat16)
    row_iota = lax.broadcasted_iota(jnp.int32, (2 * rest, LANES), 0)
    blocks = [(ref, b) for ref, picks in in_refs for b in picks]
    for n, (ref, b) in enumerate(blocks):
        pieces, lows = [], []
        for j in range(chunks):
            tail = whole * chunks + j * rest
            main_top, main_rest = split(ref[b, pl.ds(j * whole, whole), :])
            end = ref[b, pl.ds(tail, rest), :]
            cell = end[members - whole + 1 : members - whole + 2].astype(jnp.int32)
            live = (cell >= 0).astype(jnp.float32)
            end = jnp.concatenate([end, end], 0)
            end = jnp.where(row_iota % rest == members - whole + 1, live, end)
            end_top, end_rest = split(end)
            end = jnp.where(row_iota < rest, end_top, end_rest)
            piece = jnp.concatenate([main_top, main_rest, end], 0)
            high = lax.shift_right_arithmetic(cell, 8)
            pieces.append([jnp.where(high == g, piece, 0.0) for g in range(GROUPS)])
            lows.append(jnp.where(low_half == (cell & (WIDE - 1)).astype(jnp.float32).astype(jnp.bfloat16), one, nil))
        left = jnp.concatenate(
            [jnp.concatenate([p[g] for p in pieces], 1) for g in range(GROUPS)], 0
        ).astype(jnp.bfloat16)
        low = jnp.concatenate(lows, 1)
        product = lax.dot_general(
            left, low, (((1,), (1,)), ((), ())), preferred_element_type=jnp.float32
        )
        if n:
            acc_ref[...] += product
        elif start_ref is None:
            acc_ref[...] = product
        else:
            acc_ref[...] = start_ref[...] + product


def finish(members, acc_ref, moment_ref, result_ref):
    rows, whole = block_rows(members)
    rest, extra = rows - whole, members - whole
    for g in range(GROUPS):
        start, width = g * WIDE, min(WIDE, CELL_DEV - g * WIDE)
        base = g * 2 * rows
        main = acc_ref[pl.ds(base, whole), :width] + acc_ref[pl.ds(base + whole, whole), :width]
        end = acc_ref[pl.ds(base + 2 * whole, 2 * rest), :width]
        end = end[:rest] + end[rest:]
        counted = end[extra + 1 : extra + 2]
        filled = counted > 0
        total = jnp.where(filled, end[extra : extra + 1], 1.0)
        inverse = 1.0 / total
        main = main * inverse
        last = end[:extra] * inverse
        moment = jnp.sum(main, 0, keepdims=True) + jnp.sum(last, 0, keepdims=True)
        mean = moment * (1.0 / members)
        main_gap, last_gap = main - mean, last - mean
        spread = jnp.sum(main_gap * main_gap, 0, keepdims=True) + jnp.sum(last_gap * last_gap, 0, keepdims=True)
        error = jnp.where(filled, inverse, 0.0)
        for j in range(width // LANES):
            line, cut = start // LANES + j, slice(j * LANES, (j + 1) * LANES)
            tail = LINES * whole + line * rest
            result_ref[line * whole : (line + 1) * whole, :] = main[:, cut]
            result_ref[tail : tail + extra, :] = last[:, cut]
            result_ref[tail + extra : tail + extra + 1, :] = error[:, cut]
            result_ref[tail + extra + 1 : tail + extra + 2, :] = counted[:, cut]
            moment_ref[0, line : line + 1, :] = moment[:, cut]
            moment_ref[1, line : line + 1, :] = spread[:, cut]


def near(array):
    return pltpu.with_memory_space_constraint(array, pltpu.VMEM)


def bin_some(members, chunks, arrays, start=None, last=False):
    acc = pltpu.VMEM((GROUPS * 2 * block_rows(members)[0], WIDE), jnp.float32)
    inputs = [array for array, _ in arrays] + ([] if start is None else [start])

    def body(*refs):
        ins, outs = refs[: len(inputs)], refs[len(inputs) :]
        start_ref = None if start is None else ins[-1]
        pairs = list(zip(ins, [picks for _, picks in arrays]))
        accumulate(members, chunks, pairs, start_ref, outs[-1])
        if last:
            finish(members, outs[-1], *outs[:-1])

    return pl.pallas_call(
        body,
        out_shape=[
            pltpu.VMEM((2, LINES, LANES), jnp.float32),
            pltpu.VMEM((LINES * block_rows(members)[0], LANES), jnp.float32),
        ]
        if last
        else acc,
        scratch_shapes=[acc] if last else [],
    )(*[near(array) for array in inputs])


def final_kernel(
    members, total, own_ref, passed_ref, moment_ref, own_count_ref, out_ref, departure_ref, variance_ref, error_ref, count_ref
):
    mean = moment_ref[0] * (1.0 / total)
    departure_ref[...] = -mean
    variance_ref[...] = moment_ref[1] * (1.0 / (total - 1))

    rows, whole = block_rows(members)
    rest, extra = rows - whole, members - whole

    def write(result_ref, own_counts=None):
        if own_counts is not None:
            count_ref[...] = own_counts[...]
        for j in range(LINES):
            cut = slice(j * LANES, (j + 1) * LANES)
            tail = LINES * whole + j * rest
            line, below = mean[j : j + 1], slice(tail + extra, tail + extra + 1)
            out_ref[:whole, cut] = result_ref[j * whole : (j + 1) * whole, :] - line
            out_ref[whole:, cut] = result_ref[tail : tail + extra, :] - line
            error_ref[j : j + 1, :] = result_ref[below, :]
            if own_counts is None:
                count_ref[j : j + 1, :] = result_ref[tail + extra + 1 : tail + extra + 2, :].astype(jnp.int32)

    odd = odd_plane()
    pl.when(odd == 0)(lambda: write(own_ref, own_count_ref))
    pl.when(odd == 1)(lambda: write(passed_ref))


def count_kernel(members, result_ref, out_ref):
    rows, whole = block_rows(members)
    for j in range(LINES):
        spot = LINES * whole + (j + 1) * (rows - whole) - 1
        out_ref[j : j + 1, :] = result_ref[spot : spot + 1, :].astype(jnp.int32)


def merge(mine, theirs, each):
    gap = mine[0] - theirs[0]
    return jnp.stack([mine[0] + theirs[0], mine[1] + theirs[1] + gap * gap / (2 * each)])


def chip_order(chips):
    return list(range(chips - 1, 0, -1))


def step(member_values, obs_value, obs_weight, obs_cell):
    regions = lax.axis_size("reg")
    groups = lax.axis_size("mem")
    members, slots = member_values.shape
    chunks = slots // regions // LANES
    chips = regions // 2
    swap = [(i, i ^ 1) for i in range(regions)]
    lines = (slots // LANES, LANES)
    shape = (chunks * block_rows(members)[0], LANES)
    same, other, direct = pl.pallas_call(
        functools.partial(pack_kernel, members, regions, chunks),
        out_shape=[pltpu.VMEM((n, *shape), jnp.float32) for n in (chips - 1, chips - 1, 2)],
    )(member_values, obs_value.reshape(lines), obs_weight.reshape(lines), obs_cell.reshape(lines))
    partner = lax.ppermute(other, "reg", swap)
    arrivals = []
    for k in chip_order(chips):
        sent = direct if k == chips - 1 else jnp.stack([same[k], partner[k]])
        pairs = [(i, i ^ (2 * k + 1)) for i in range(regions)]
        arrivals.append((lax.ppermute(sent, "reg", pairs), (0, 1)))
    landed = arrivals[0][0]
    forwarded = (lax.ppermute(landed, "reg", swap), (1,))
    sums = bin_some(members, chunks, [(same, (0,)), (partner, (0,))])
    sums = bin_some(members, chunks, [(landed, (0,))], sums)
    sums = bin_some(members, chunks, [forwarded], sums)
    sums = bin_some(members, chunks, arrivals[1:], sums, True)
    moments, own = sums
    passed = lax.ppermute(own, "reg", swap)
    counts = pl.pallas_call(
        functools.partial(count_kernel, members), out_shape=pltpu.VMEM((LINES, LANES), jnp.int32)
    )(near(own))
    each, reach = members, 1
    while reach < groups:
        pairs = [(z * regions + i, (z ^ reach) * regions + (i ^ 1)) for z in range(groups) for i in range(regions)]
        theirs = lax.ppermute(moments, ("mem", "reg"), pairs)
        moments = merge(moments, theirs, each)
        each, reach = 2 * each, 2 * reach
    moments = lax.cond(odd_plane() == 1, lambda m: lax.ppermute(m, "reg", swap), lambda m: m, moments)
    cells = jax.ShapeDtypeStruct((LINES, LANES), jnp.float32)
    outs = pl.pallas_call(
        functools.partial(final_kernel, members, members * groups),
        out_shape=[
            jax.ShapeDtypeStruct((members, CELL_DEV), jnp.float32),
            cells,
            cells,
            cells,
            jax.ShapeDtypeStruct((LINES, LANES), jnp.int32),
        ],
    )(*[near(a) for a in (own, passed, moments, counts)])
    return (outs[0], *[out.reshape(-1) for out in outs[1:]])


def solution(mesh):
    return jax.shard_map(
        step,
        mesh=mesh,
        in_specs=(P("mem", "reg"), P("reg"), P("reg"), P("reg")),
        out_specs=(P("mem", "reg"), P("reg"), P("reg"), P("reg"), P("reg")),
        check_vma=False,
    )
```

```python
import functools
import jax
import jax.numpy as jnp
from jax import lax
from jax.experimental import pallas as pl
from jax.experimental.pallas import tpu as pltpu
from jax.sharding import PartitionSpec as P

CELL_DEV = 1920
LANES = 128
WIDE = 256
LINES = CELL_DEV // LANES
GROUPS = -(-CELL_DEV // WIDE)


def round_up(size, unit):
    return -(-size // unit) * unit


def block_rows(members):
    rows = round_up(members + 2, 4)
    return rows, rows // 8 * 8


def odd_plane():
    plane = lax.axis_index("mem")
    odd = plane & 1
    for bit in range(1, lax.axis_size("mem").bit_length() - 1):
        odd = odd ^ (lax.shift_right_logical(plane, bit) & 1)
    return odd


def pack_kernel(members, regions, chunks, value_ref, obs_ref, weight_ref, cell_ref, same_ref, other_ref, direct_ref):
    me, odd = lax.axis_index("reg"), odd_plane()
    rows, whole = block_rows(members)
    rest = rows - whole
    for step in range(regions):
        owner = me ^ step ^ odd
        if step // 2 == regions // 2 - 1:
            out_ref, slot = direct_ref, 1 - step % 2
        else:
            out_ref, slot = other_ref if (step % 2) ^ (step > 1) else same_ref, step // 2
        for j in range(chunks):
            line = owner * chunks + j
            values = value_ref[:, pl.ds(pl.multiple_of(line * LANES, LANES), LANES)]
            cell = cell_ref[pl.ds(line, 1), :]
            live = cell >= 0
            weight = jnp.where(live, weight_ref[pl.ds(line, 1), :], 0.0)
            local = jnp.where(live, cell - owner * CELL_DEV, -1).astype(jnp.float32)
            innovation = (values - obs_ref[pl.ds(line, 1), :]) * weight
            tail = whole * chunks + j * rest
            out_ref[slot, pl.ds(j * whole, whole), :] = innovation[:whole]
            out_ref[slot, pl.ds(tail, members - whole), :] = innovation[whole:]
            out_ref[slot, pl.ds(tail + members - whole, 1), :] = weight
            out_ref[slot, pl.ds(tail + members - whole + 1, 1), :] = local


def split(values):
    top = values.astype(jnp.bfloat16).astype(jnp.float32)
    return top, (values - top).astype(jnp.bfloat16).astype(jnp.float32)


def accumulate(members, chunks, in_refs, start_ref, acc_ref):
    rows, whole = block_rows(members)
    rest = rows - whole
    low_iota = lax.broadcasted_iota(jnp.int32, (WIDE, LANES), 0)
    low_half = low_iota.astype(jnp.float32).astype(jnp.bfloat16)
    one, nil = jnp.ones((), jnp.bfloat16), jnp.zeros((), jnp.bfloat16)
    row_iota = lax.broadcasted_iota(jnp.int32, (2 * rest, LANES), 0)
    blocks = [(ref, b) for ref, picks in in_refs for b in picks]
    for n, (ref, b) in enumerate(blocks):
        pieces, lows = [], []
        for j in range(chunks):
            tail = whole * chunks + j * rest
            main_top, main_rest = split(ref[b, pl.ds(j * whole, whole), :])
            end = ref[b, pl.ds(tail, rest), :]
            cell = end[members - whole + 1 : members - whole + 2].astype(jnp.int32)
            live = (cell >= 0).astype(jnp.float32)
            end = jnp.concatenate([end, end], 0)
            end = jnp.where(row_iota % rest == members - whole + 1, live, end)
            end_top, end_rest = split(end)
            end = jnp.where(row_iota < rest, end_top, end_rest)
            piece = jnp.concatenate([main_top, main_rest, end], 0)
            high = lax.shift_right_arithmetic(cell, 8)
            pieces.append([jnp.where(high == g, piece, 0.0) for g in range(GROUPS)])
            lows.append(jnp.where(low_half == (cell & (WIDE - 1)).astype(jnp.float32).astype(jnp.bfloat16), one, nil))
        left = jnp.concatenate(
            [jnp.concatenate([p[g] for p in pieces], 1) for g in range(GROUPS)], 0
        ).astype(jnp.bfloat16)
        low = jnp.concatenate(lows, 1)
        product = lax.dot_general(
            left, low, (((1,), (1,)), ((), ())), preferred_element_type=jnp.float32
        )
        if n:
            acc_ref[...] += product
        elif start_ref is None:
            acc_ref[...] = product
        else:
            acc_ref[...] = start_ref[...] + product


def finish(members, acc_ref, moment_ref, result_ref):
    rows, whole = block_rows(members)
    rest, extra = rows - whole, members - whole
    for g in range(GROUPS):
        start, width = g * WIDE, min(WIDE, CELL_DEV - g * WIDE)
        base = g * 2 * rows
        main = acc_ref[pl.ds(base, whole), :width] + acc_ref[pl.ds(base + whole, whole), :width]
        end = acc_ref[pl.ds(base + 2 * whole, 2 * rest), :width]
        end = end[:rest] + end[rest:]
        counted = end[extra + 1 : extra + 2]
        filled = counted > 0
        total = jnp.where(filled, end[extra : extra + 1], 1.0)
        inverse = 1.0 / total
        main = main * inverse
        last = end[:extra] * inverse
        moment = jnp.sum(main, 0, keepdims=True) + jnp.sum(last, 0, keepdims=True)
        mean = moment * (1.0 / members)
        main_gap, last_gap = main - mean, last - mean
        spread = jnp.sum(main_gap * main_gap, 0, keepdims=True) + jnp.sum(last_gap * last_gap, 0, keepdims=True)
        error = jnp.where(filled, inverse, 0.0)
        for j in range(width // LANES):
            line, cut = start // LANES + j, slice(j * LANES, (j + 1) * LANES)
            tail = LINES * whole + line * rest
            result_ref[line * whole : (line + 1) * whole, :] = main[:, cut]
            result_ref[tail : tail + extra, :] = last[:, cut]
            result_ref[tail + extra : tail + extra + 1, :] = error[:, cut]
            result_ref[tail + extra + 1 : tail + extra + 2, :] = counted[:, cut]
            moment_ref[0, line : line + 1, :] = moment[:, cut]
            moment_ref[1, line : line + 1, :] = spread[:, cut]


def near(array):
    return pltpu.with_memory_space_constraint(array, pltpu.VMEM)


def bin_some(members, chunks, arrays, start=None, last=False):
    acc = pltpu.VMEM((GROUPS * 2 * block_rows(members)[0], WIDE), jnp.float32)
    inputs = [array for array, _ in arrays] + ([] if start is None else [start])

    def body(*refs):
        ins, outs = refs[: len(inputs)], refs[len(inputs) :]
        start_ref = None if start is None else ins[-1]
        pairs = list(zip(ins, [picks for _, picks in arrays]))
        accumulate(members, chunks, pairs, start_ref, outs[-1])
        if last:
            finish(members, outs[-1], *outs[:-1])

    return pl.pallas_call(
        body,
        out_shape=[
            pltpu.VMEM((2, LINES, LANES), jnp.float32),
            pltpu.VMEM((LINES * block_rows(members)[0], LANES), jnp.float32),
        ]
        if last
        else acc,
        scratch_shapes=[acc] if last else [],
    )(*[near(array) for array in inputs])


def final_kernel(
    members, total, own_ref, passed_ref, moment_ref, own_count_ref, out_ref, departure_ref, variance_ref, error_ref, count_ref
):
    mean = moment_ref[0] * (1.0 / total)
    departure_ref[...] = -mean
    variance_ref[...] = moment_ref[1] * (1.0 / (total - 1))

    rows, whole = block_rows(members)
    rest, extra = rows - whole, members - whole

    def write(result_ref, own_counts=None):
        if own_counts is not None:
            count_ref[...] = own_counts[...]
        for j in range(LINES):
            cut = slice(j * LANES, (j + 1) * LANES)
            tail = LINES * whole + j * rest
            line, below = mean[j : j + 1], slice(tail + extra, tail + extra + 1)
            out_ref[:whole, cut] = result_ref[j * whole : (j + 1) * whole, :] - line
            out_ref[whole:, cut] = result_ref[tail : tail + extra, :] - line
            error_ref[j : j + 1, :] = result_ref[below, :]
            if own_counts is None:
                count_ref[j : j + 1, :] = result_ref[tail + extra + 1 : tail + extra + 2, :].astype(jnp.int32)

    odd = odd_plane()
    pl.when(odd == 0)(lambda: write(own_ref, own_count_ref))
    pl.when(odd == 1)(lambda: write(passed_ref))


def count_kernel(members, result_ref, out_ref):
    rows, whole = block_rows(members)
    for j in range(LINES):
        spot = LINES * whole + (j + 1) * (rows - whole) - 1
        out_ref[j : j + 1, :] = result_ref[spot : spot + 1, :].astype(jnp.int32)


def merge(mine, theirs, each):
    gap = mine[0] - theirs[0]
    return jnp.stack([mine[0] + theirs[0], mine[1] + theirs[1] + gap * gap / (2 * each)])


def chip_order(chips):
    return list(range(chips - 1, 0, -1))


def step(member_values, obs_value, obs_weight, obs_cell):
    regions = lax.axis_size("reg")
    groups = lax.axis_size("mem")
    members, slots = member_values.shape
    chunks = slots // regions // LANES
    chips = regions // 2
    swap = [(i, i ^ 1) for i in range(regions)]
    lines = (slots // LANES, LANES)
    shape = (chunks * block_rows(members)[0], LANES)
    same, other, direct = pl.pallas_call(
        functools.partial(pack_kernel, members, regions, chunks),
        out_shape=[pltpu.VMEM((n, *shape), jnp.float32) for n in (chips - 1, chips - 1, 2)],
    )(member_values, obs_value.reshape(lines), obs_weight.reshape(lines), obs_cell.reshape(lines))
    partner = lax.ppermute(other, "reg", swap)
    arrivals = []
    for k in chip_order(chips):
        sent = direct if k == chips - 1 else jnp.stack([same[k], partner[k]])
        pairs = [(i, i ^ (2 * k + 1)) for i in range(regions)]
        arrivals.append((lax.ppermute(sent, "reg", pairs), (0, 1)))
    landed = arrivals[0][0]
    forwarded = (lax.ppermute(landed, "reg", swap), (1,))
    sums = bin_some(members, chunks, [(same, (0,)), (partner, (0,))])
    sums = bin_some(members, chunks, [(landed, (0,))], sums)
    sums = bin_some(members, chunks, [forwarded], sums)
    sums = bin_some(members, chunks, arrivals[1:], sums, True)
    moments, own = sums
    passed = lax.ppermute(own, "reg", swap)
    counts = pl.pallas_call(
        functools.partial(count_kernel, members), out_shape=pltpu.VMEM((LINES, LANES), jnp.int32)
    )(near(own))
    each, reach = members, groups // 2
    while reach:
        pairs = [(z * regions + i, (z ^ reach) * regions + (i ^ 1)) for z in range(groups) for i in range(regions)]
        theirs = lax.ppermute(moments, ("mem", "reg"), pairs)
        moments = merge(moments, theirs, each)
        each, reach = 2 * each, reach // 2
    moments = lax.cond(odd_plane() == 1, lambda m: lax.ppermute(m, "reg", swap), lambda m: m, moments)
    cells = jax.ShapeDtypeStruct((LINES, LANES), jnp.float32)
    outs = pl.pallas_call(
        functools.partial(final_kernel, members, members * groups),
        out_shape=[
            jax.ShapeDtypeStruct((members, CELL_DEV), jnp.float32),
            cells,
            cells,
            cells,
            jax.ShapeDtypeStruct((LINES, LANES), jnp.int32),
        ],
    )(*[near(a) for a in (own, passed, moments, counts)])
    return (outs[0], *[out.reshape(-1) for out in outs[1:]])


def solution(mesh):
    return jax.shard_map(
        step,
        mesh=mesh,
        in_specs=(P("mem", "reg"), P("reg"), P("reg"), P("reg")),
        out_specs=(P("mem", "reg"), P("reg"), P("reg"), P("reg"), P("reg")),
        check_vma=False,
    )
```
